32 devices in a mesh: depth: 8 (over z, core), gx: 4 (over y, x).
Axes of the slice: x: 2, y: 2, z: 4, core: 2. Of those that a mesh axis runs over, the one named last changes fastest.
Arguments:
- pressure_now: float32 [4, 128, 256, 128], P(None, 'gx', 'depth'), may hold values from -6 to 6
- pressure_before: float32 [4, 128, 256, 128], P(None, 'gx', 'depth'), may hold values from -6 to 6
- class_map: int32 [128, 256, 128], P('gx', 'depth'), may hold values from 0 to 7
- courant_sq: float32 [8], replicated, may hold values from 0.02 to 0.12
- source_cells: int32 [4, 3], replicated, may hold values from 0 to 255, as said below
- source_wavelet: float32 [8, 4], replicated, may hold values from -6 to 6
- layer_start: int32 [1], replicated, may hold values from 232 to 240
Outputs:
- pressure_final: float32 [4, 128, 256, 128], P(None, 'gx', 'depth')
- pressure_prior: float32 [4, 128, 256, 128], P(None, 'gx', 'depth')
The draws below stay inside these ranges and needn't reach their ends.
Inputs may be any that keep to these rules, and one draw needn't show every extreme that they name: `source_cells`: each row holds a cell inside the grid: x below 128, depth below 256, y below 128; shot 0 sits at the last cell along every dimension and shot 1 at cell (0, 0, 0).
All inputs are finite; a program needn't handle non-finite values.
Results may differ from the reference program's by a relative error of at most 0.00002.
Values sent between devices are 32-bit elements; how exact they have to be, the bound alone decides.
A program may use at most 128 MiB of HBM per device.

```python
import math
import jax
import jax.numpy as jnp

NY = 128
SHOTS = 4
ITERS = 8
CLASSES = 8
NX = 128
NZ = 256


def draw_source_cells(key, part):
    key_x = jax.random.fold_in(key, 11)
    key_z = jax.random.fold_in(key, 12)
    key_y = jax.random.fold_in(key, 13)
    cell_x = jax.random.randint(key_x, (SHOTS,), 0, NX, dtype=jnp.int32)
    cell_z = jax.random.randint(key_z, (SHOTS,), 0, NZ, dtype=jnp.int32)
    cell_y = jax.random.randint(key_y, (SHOTS,), 0, NY, dtype=jnp.int32)
    cell_x = cell_x.at[0].set(jnp.int32(NX - 1)).at[1].set(jnp.int32(0))
    cell_z = cell_z.at[0].set(jnp.int32(NZ - 1)).at[1].set(jnp.int32(0))
    cell_y = cell_y.at[0].set(jnp.int32(NY - 1)).at[1].set(jnp.int32(0))
    return jnp.stack([cell_x, cell_z, cell_y], axis=1)


def plant(entries, own_key, low, top_value):
    longest = entries.shape.index(max(entries.shape))
    spots = []
    for shift in (0, 1):
        where = [jax.random.randint(jax.random.fold_in(own_key, axis), (), 0, length) for axis, length in enumerate(entries.shape)]
        where[longest] = (where[longest] + shift) % entries.shape[longest]
        spots.append(tuple(where))
    return entries.at[spots[0]].set(low).at[spots[1]].set(top_value)


def block_scale(key, dims, shards, smallest, top_value):
    def one(axis_at, blocks):
        draws = jax.random.uniform(jax.random.fold_in(jax.random.fold_in(key, 6), axis_at), (blocks,), jnp.float32, smallest / len(shards), top_value / len(shards))
        return jnp.repeat(jnp.exp(draws), dims[axis_at] // blocks).reshape((-1,) + (1,) * (len(dims) - axis_at - 1))

    gain = one(*shards[0])
    for cut in shards[1:]:
        gain = gain * one(*cut)
    return gain


def noise(stream_key, dims, spread, bound, cuts=(), kind=jnp.bfloat16):
    drawn = jax.random.normal(stream_key, dims, jnp.float32) * spread
    if len(cuts) > 0:
        drawn = block_scale(stream_key, dims, cuts, -0.22, 0.18) * drawn
    return jnp.clip(drawn, min=-bound, max=bound).astype(kind)


def setup_inputs(seed: int = 0) -> dict:
    key_of = jax.random.split(jax.random.key(seed), 8)
    pressure_now = noise(key_of[0], (SHOTS, NX, NZ, NY), 1.0, 6.0, ((1, 4), (2, 8)), jnp.float32)
    pressure_before = noise(key_of[1], (SHOTS, NX, NZ, NY), 1.0, 6.0, ((1, 4), (2, 8)), jnp.float32)
    class_map = plant(jax.random.randint(key_of[2], (NX, NZ, NY), 0, CLASSES), jax.random.fold_in(key_of[2], 1), 0, CLASSES - 1).astype(jnp.int32)
    courant_sq = jnp.clip(jnp.exp(jax.random.uniform(key_of[3], (CLASSES,), jnp.float32, math.log(0.02), math.log(0.12))), 0.02, 0.12)
    source_cells = draw_source_cells(jax.random.fold_in(key_of[7], 71), 0)
    source_wavelet = noise(key_of[5], (ITERS, SHOTS), 1.0, 6.0, (), jnp.float32)
    layer_start = jax.random.randint(key_of[6], (1,), NZ - 24, NZ - 15).astype(jnp.int32)
    return dict(pressure_now=pressure_now, pressure_before=pressure_before, class_map=class_map, courant_sq=courant_sq, source_cells=source_cells, source_wavelet=source_wavelet, layer_start=layer_start)


COEFFS = (-205.0 / 72.0, 8.0 / 5.0, -1.0 / 5.0, 8.0 / 315.0, -1.0 / 560.0)
DAMPING = 0.3


def laplace(padded, rows, depth):
    center = padded[:, 4:4 + rows, 4:4 + depth, :]
    total = 3.0 * COEFFS[0] * center
    side_y = jnp.pad(center, ((0, 0), (0, 0), (0, 0), (4, 4)))
    width = center.shape[3]
    for k in range(1, 5):
        pair = padded[:, 4 + k:4 + k + rows, 4:4 + depth, :] + padded[:, 4 - k:4 - k + rows, 4:4 + depth, :]
        pair = pair + padded[:, 4:4 + rows, 4 + k:4 + k + depth, :] + padded[:, 4:4 + rows, 4 - k:4 - k + depth, :]
        pair = pair + side_y[:, :, :, 4 + k:4 + k + width] + side_y[:, :, :, 4 - k:4 - k + width]
        total = total + COEFFS[k] * pair
    return total


def advance(current, before, padded, speed, damping, source):
    lap = laplace(padded, current.shape[1], current.shape[2])
    return (2.0 * current - (1.0 - damping) * before + speed * lap + source) / (1.0 + damping)


def profile(global_z, start, total):
    ratio = (global_z - start + 1).astype(jnp.float32) / (total - start).astype(jnp.float32)
    return jnp.where(global_z >= start, DAMPING * ratio * ratio, jnp.float32(0.0))


def point_mask(cells, column, anchor, count):
    index = anchor + jnp.arange(count, dtype=jnp.int32)
    return (index[None, :] == cells[:, column][:, None]).astype(jnp.float32)


def reference(pressure_now, pressure_before, class_map, courant_sq, source_cells, source_wavelet, layer_start):
    speed = courant_sq[class_map]
    depth_index = jnp.arange(NZ, dtype=jnp.int32)
    damping = profile(depth_index, layer_start[0], jnp.int32(NZ))[None, None, :, None]
    mask_x = point_mask(source_cells, 0, jnp.int32(0), NX)
    mask_z = point_mask(source_cells, 1, jnp.int32(0), NZ)
    mask_y = point_mask(source_cells, 2, jnp.int32(0), NY)
    onehot = mask_x[:, :, None, None] * mask_z[:, None, :, None] * mask_y[:, None, None, :]
    current, before = pressure_now, pressure_before
    for step in range(ITERS):
        padded = jnp.pad(current, ((0, 0), (4, 4), (4, 4), (0, 0)))
        source = source_wavelet[step][:, None, None, None] * onehot
        nxt = advance(current, before, padded, speed, damping, source)
        before, current = current, nxt
    return current, before
```

```python
import functools
import math

import jax
import jax.numpy as jnp
from jax import lax
from jax.experimental import pallas as pl
from jax.experimental.pallas import tpu as pltpu
from jax.sharding import PartitionSpec as P

COEFFS = (-205.0 / 72.0, 8.0 / 5.0, -1.0 / 5.0, 8.0 / 315.0, -1.0 / 560.0)
DAMPING = 0.3
GROUP = 8
W = 4
T = 8
LAG = 1
DIRS = (("depth", -1), ("depth", 1), ("gx", -1), ("gx", 1))
MESH = pl.DeviceIdType.MESH


def kernel(
    sizes, side, iters, shots, rows, depth, width, classes,
    now_hbm, before_hbm, class_hbm, courant, cells, wavelet, start,
    grid,
    relay, speed, scale, klass, load_sem, class_sem,
    send_sem, recv_sem, relay_sem, forward_sem,
):
    place = {axis: lax.axis_index(axis) for axis in ("depth", "gx")}
    me = place["gx"]
    lanes = sizes["gx"]
    has = []
    for axis, delta in DIRS:
        has.append(place[axis] > 0 if delta < 0 else place[axis] < sizes[axis] - 1)

    def along(g):
        return (place["depth"], g)

    def target(d):
        axis, delta = DIRS[d]
        there = dict(place)
        there[axis] = place[axis] + delta
        return (there["depth"], there["gx"])

    relayed = side > 1
    if relayed:
        column = lax.rem(me, side)
        cross = {2: has[2] & (column == 0), 3: has[3] & (column == side - 1)}
        via = {2: me - side, 3: me + side}
        serves = {
            2: (column == 0) & (me + side < lanes),
            3: (column == side - 1) & (me - side >= 0),
        }
        serve_from = {2: me + side, 3: me - side}
        serve_to = {2: me + side - 1, 3: me - side + 1}

    half = max(T, depth // 2 // T * T) if relayed else depth

    xs, zs = pl.ds(W, rows), pl.ds(T, depth)
    za, zb = pl.ds(T, half), pl.ds(T + half, depth - half)

    def load(source, buf, s, k):
        return pltpu.make_async_copy(
            source.at[s], grid.at[buf, s, xs, zs, :], load_sem.at[k, s]
        )

    for s in range(shots):
        load(now_hbm, 0, s, 0).start()
    load_class = pltpu.make_async_copy(class_hbm, klass, class_sem)
    load_class.start()
    for s in range(shots):
        load(before_hbm, 1, s, 1).start()

    pieces = [
        (0, xs, pl.ds(T, T), xs, pl.ds(T + depth, T)),
        (1, xs, pl.ds(depth, T), xs, pl.ds(0, T)),
        (2, pl.ds(W, W), za, pl.ds(W + rows, W), za),
        (3, pl.ds(rows, W), za, pl.ds(0, W), za),
    ]
    if relayed:
        pieces += [
            (2, pl.ds(W, W), zb, pl.ds(W + rows, W), zb),
            (3, pl.ds(rows, W), zb, pl.ds(0, W), zb),
        ]

    def halo(buf, s, k):
        d, sx, sz, dx, dz = pieces[k]
        return pltpu.make_async_remote_copy(
            src_ref=grid.at[buf, s, sx, sz, :],
            dst_ref=grid.at[buf, s, dx, dz, :],
            send_sem=send_sem.at[buf, s, k],
            recv_sem=recv_sem.at[buf, s, k],
            device_id=target(d),
            device_id_type=MESH,
        )

    def detour(r, buf, s, k):
        d, sx, sz, _, _ = pieces[k]
        return pltpu.make_async_remote_copy(
            src_ref=grid.at[buf, s, sx, sz, :],
            dst_ref=relay.at[r, s],
            send_sem=send_sem.at[buf, s, k],
            recv_sem=relay_sem.at[r, s],
            device_id=along(via[d]),
            device_id_type=MESH,
        )

    def forward(r, buf, s, k):
        d, _, _, dx, dz = pieces[k]
        return pltpu.make_async_remote_copy(
            src_ref=relay.at[r, s],
            dst_ref=grid.at[buf, s, dx, dz, :],
            send_sem=forward_sem.at[r, s],
            recv_sem=recv_sem.at[buf, s, k],
            device_id=along(serve_to[d]),
            device_id_type=MESH,
        )

    for d in range(4):
        _, _, _, dx, dz = pieces[d ^ 1]
        if d >= 2:
            dz = zs

        @pl.when(jnp.logical_not(has[d]))
        def _():
            for buf in range(2):
                def clear(s, c):
                    shape = (dx.size, dz.size, width)
                    grid[buf, s, dx, dz, :] = jnp.zeros(shape, jnp.float32)
                    return c
                lax.fori_loop(0, shots, clear, 0)

    meets = [(has[d], target(d)) for d in range(4)]
    if relayed:
        for d in (2, 3):
            step_back = -side + 1 if d == 2 else side - 1
            back = me - step_back - (1 if d == 2 else -1)
            meets.append((cross[d], along(via[d])))
            meets.append((serves[d], along(serve_from[d])))
            if side > 2:
                meets.append((serves[d], along(serve_to[d])))
                meets.append((cross[d], along(me + (side - 1 if d == 2 else 1 - side))))

    barrier = pltpu.get_barrier_semaphore()
    for there, device in meets:
        @pl.when(there)
        def _():
            pl.semaphore_signal(barrier, inc=1, device_id=device, device_id_type=MESH)
    peers = sum(there.astype(jnp.int32) for there, _ in meets)
    pl.semaphore_wait(barrier, peers)

    def each(ways, straight, around):
        for k in ways:
            d = pieces[k][0]
            if k < 4:
                pl.when(has[d])(lambda: straight(k))
            else:
                pl.when(cross[d])(lambda: around(k))
                pl.when(has[d] & jnp.logical_not(cross[d]))(lambda: straight(k))

    wide = (4, 5, 2, 3) if relayed else (2, 3)

    def send(r, buf, s, ways):
        each(ways, lambda k: halo(buf, s, k).start(), lambda k: detour(r, buf, s, k).start())

    def wait_sent(buf, s):
        each(wide + (0, 1), lambda k: halo(buf, s, k).wait_send(),
             lambda k: detour(0, buf, s, k).wait_send())

    def wait_halo(buf, s):
        for k in wide + (0, 1):
            pl.when(has[pieces[k][0] ^ 1])(lambda: halo(buf, s, k).wait_recv())

    def pass_on(r, s):
        if not relayed:
            return
        for k in (4, 5):
            @pl.when(serves[pieces[k][0]])
            def _():
                buf = r % 2 if isinstance(r, int) else lax.rem(r, 2)
                detour(r, buf, s, k).wait_recv()
                forward(r, buf, s, k).start()

    for s in range(shots):
        load(now_hbm, 0, s, 0).wait()
        send(0, 0, s, wide + (0, 1))

    z_index = place["depth"] * depth + lax.broadcasted_iota(jnp.int32, (depth, width), 0)
    total = depth * sizes["depth"]
    begin = jnp.full((depth, width), start[0], jnp.int32)
    ratio = (z_index - begin + 1).astype(jnp.float32) / (total - begin).astype(jnp.float32)
    damping = jnp.where(z_index >= begin, DAMPING * ratio * ratio, jnp.float32(0.0))
    inverse = 1.0 / (1.0 + damping)
    scale[0] = inverse
    scale[1] = 2.0 * inverse

    load_class.wait()

    def lookup(x, c):
        held = klass[x]
        value = jnp.zeros((depth, width), jnp.float32)
        for k in range(classes):
            value = jnp.where(held == k, courant[k], value)
        speed[x] = value * scale[0]
        return c

    lax.fori_loop(0, rows, lookup, 0)
    for s in range(shots):
        load(before_hbm, 1, s, 1).wait()

    lag = min(LAG, shots)
    for s in range(shots - lag):
        pass_on(0, s)

    lane = lax.broadcasted_iota(jnp.int32, (T, width), 1)
    low = [jnp.where(lane >= k, jnp.float32(COEFFS[k]), 0.0) for k in range(1, W + 1)]
    high = [jnp.where(lane < width - k, jnp.float32(COEFFS[k]), 0.0) for k in range(1, W + 1)]
    x_anchor = place["gx"] * rows

    def compute(t, s, buf, other):
        lane_z = lax.broadcasted_iota(jnp.int32, (depth, width), 1)
        hit = (z_index == cells[s, 1]) & (lane_z == cells[s, 2])
        pulse = jnp.where(hit, wavelet[s, t] * scale[0], 0.0)
        cell_x = cells[s, 0] - x_anchor

        group = math.gcd(rows, GROUP)

        def block_of(x, j):
            z = T + j * T

            def at(dx, dz):
                return grid[buf, s, x + W + dx, pl.ds(z + dz, T), :]

            p = at(0, 0)
            lap = (3.0 * COEFFS[0]) * p
            for k in range(1, W + 1):
                pair = (at(k, 0) + at(-k, 0)) + (at(0, k) + at(0, -k))
                lap = lap + COEFFS[k] * pair
                lap = lap + (
                    low[k - 1] * pltpu.roll(p, k, 1)
                    + high[k - 1] * pltpu.roll(p, width - k, 1)
                )
            q = grid[other, s, x + W, pl.ds(z, T), :]
            block = pl.ds(j * T, T)
            nxt = scale[1, block, :] * (p - q) + q + speed[x, block, :] * lap
            amp = jnp.where(x == cell_x, jnp.float32(1.0), jnp.float32(0.0))
            return nxt + amp * pulse[j * T : (j + 1) * T]

        def row(g, c):
            spots = [(g * group + i, j) for i in range(group) for j in range(depth // T)]
            values = [block_of(x, j) for x, j in spots]
            for (x, j), value in zip(spots, values):
                grid[other, s, x + W, pl.ds(T + j * T, T), :] = value
            return c

        count = rows // group
        edges = min(count, 2)
        lax.fori_loop(0, edges, lambda g, c: row(g * (count - 1), c), 0)

        @pl.when(t < iters - 1)
        def _():
            send(t + 1, other, s, wide)

        lax.fori_loop(1, count - 1, row, 0)

    def step(t, c):
        buf = lax.rem(t, 2)
        other = 1 - buf

        def shot(s, c):
            wait_halo(buf, s)

            @pl.when(t >= 1)
            def _():
                wait_sent(other, s)

            compute(t, s, buf, other)

            @pl.when(t < iters - 1)
            def _():
                send(t + 1, other, s, (0, 1))

            unit = t * shots + s + shots - lag
            r, u = unit // shots, lax.rem(unit, shots)

            @pl.when(r < iters)
            def _():
                pass_on(r, u)

            return c

        return lax.fori_loop(0, shots, shot, c)

    lax.fori_loop(0, iters, step, 0)
    for s in range(shots):
        wait_sent(1 - iters % 2, s)
    if relayed:
        for k in (4, 5):
            @pl.when(serves[pieces[k][0]])
            def _():
                def gone(i, c):
                    r = i // shots
                    forward(r, lax.rem(r, 2), lax.rem(i, shots), k).wait_send()
                    return c
                lax.fori_loop(0, iters * shots, gone, 0)


def put_out(iters, shots, rows, depth, grid, final_hbm, prior_hbm, out_sem):
    xs, zs = pl.ds(W, rows), pl.ds(T, depth)
    copies = [
        pltpu.make_async_copy(grid.at[buf, s, xs, zs, :], out.at[s], out_sem.at[k, s])
        for s in range(shots)
        for k, (buf, out) in enumerate(((iters % 2, final_hbm), (1 - iters % 2, prior_hbm)))
    ]
    for copy in copies:
        copy.start()
    for copy in copies:
        copy.wait()


def solution(mesh):
    sizes = {axis: mesh.shape[axis] for axis in ("depth", "gx")}
    side = math.isqrt(sizes["gx"])
    if side * side != sizes["gx"]:
        side = 0

    def local(now, before, class_map, courant, cells, wavelet, start):
        shots, rows, depth, width = now.shape
        iters = wavelet.shape[0]
        split = side if depth >= 2 * T else 0
        body = functools.partial(
            kernel, sizes, split, iters, shots, rows, depth, width, courant.shape[0]
        )
        whole = pl.BlockSpec(memory_space=pl.ANY)
        far = pl.BlockSpec(memory_space=pltpu.HBM)
        scalar = pl.BlockSpec(memory_space=pltpu.SMEM)
        out = jax.ShapeDtypeStruct(now.shape, jnp.float32)
        half = max(T, depth // 2 // T * T)
        now, before, class_map = (
            pltpu.with_memory_space_constraint(a, pltpu.HBM) for a in (now, before, class_map)
        )
        grid = pl.pallas_call(
            body,
            out_shape=pltpu.VMEM(
                (2, shots, rows + 2 * W, depth + 2 * T, width), jnp.float32
            ),
            in_specs=[far] * 3 + [scalar] * 4,
            out_specs=pl.BlockSpec(memory_space=pltpu.VMEM),
            scratch_shapes=[
                pltpu.VMEM((iters, shots, W, depth - half, width), jnp.float32),
                pltpu.VMEM((rows, depth, width), jnp.float32),
                pltpu.VMEM((2, depth, width), jnp.float32),
                pltpu.VMEM((rows, depth, width), jnp.int32),
                pltpu.SemaphoreType.DMA((2, shots)),
                pltpu.SemaphoreType.DMA,
                pltpu.SemaphoreType.DMA((2, shots, 6)),
                pltpu.SemaphoreType.DMA((2, shots, 6)),
                pltpu.SemaphoreType.DMA((iters, shots)),
                pltpu.SemaphoreType.DMA((iters, shots)),
            ],
            compiler_params=pltpu.CompilerParams(
                collective_id=0, has_side_effects=True, vmem_limit_bytes=16 * 1024 * 1024
            ),
            name="wave",
        )(now, before, class_map, courant, cells, wavelet.T, start)
        grid = pltpu.with_memory_space_constraint(grid, pltpu.VMEM)
        return pl.pallas_call(
            functools.partial(put_out, iters, shots, rows, depth),
            out_shape=(out, out),
            in_specs=[whole],
            out_specs=(whole, whole),
            scratch_shapes=[pltpu.SemaphoreType.DMA((2, shots))],
            compiler_params=pltpu.CompilerParams(vmem_limit_bytes=1024 * 1024),
            name="put_out",
        )(grid)

    placed = P(None, "gx", "depth", None)
    return jax.shard_map(
        local,
        mesh=mesh,
        in_specs=(placed, placed, P("gx", "depth", None), P(), P(), P(), P()),
        out_specs=(placed, placed),
        check_vma=False,
    )
```

```python
import functools
import math

import jax
import jax.numpy as jnp
from jax import lax
from jax.experimental import pallas as pl
from jax.experimental.pallas import tpu as pltpu
from jax.sharding import PartitionSpec as P

COEFFS = (-205.0 / 72.0, 8.0 / 5.0, -1.0 / 5.0, 8.0 / 315.0, -1.0 / 560.0)
DAMPING = 0.3
GROUP = 8
W = 4
T = 8
LAG = 2
ZL = W
DIRS = (("depth", -1), ("depth", 1), ("gx", -1), ("gx", 1))
MESH = pl.DeviceIdType.MESH


def kernel(
    sizes, side, iters, shots, rows, depth, width, classes,
    now_hbm, before_hbm, class_hbm, courant_hbm, cells_hbm, wavelet_hbm, start,
    grid,
    courant, cells, wavelet, scalar_sem,
    relay, speed, scale, klass, load_sem, class_sem,
    send_sem, recv_sem, relay_sem, forward_sem,
):
    place = {axis: lax.axis_index(axis) for axis in ("depth", "gx")}
    me = place["gx"]
    lanes = sizes["gx"]
    has = []
    for axis, delta in DIRS:
        has.append(place[axis] > 0 if delta < 0 else place[axis] < sizes[axis] - 1)

    def along(g):
        return (place["depth"], g)

    def target(d):
        axis, delta = DIRS[d]
        there = dict(place)
        there[axis] = place[axis] + delta
        return (there["depth"], there["gx"])

    relayed = side > 1
    if relayed:
        column = lax.rem(me, side)
        cross = {2: has[2] & (column == 0), 3: has[3] & (column == side - 1)}
        via = {2: me - side, 3: me + side}
        serves = {
            2: (column == 0) & (me + side < lanes),
            3: (column == side - 1) & (me - side >= 0),
        }
        serve_from = {2: me + side, 3: me - side}
        serve_to = {2: me + side - 1, 3: me - side + 1}

    half = max(T, depth // 2 // T * T) if relayed else depth

    xs, zs = pl.ds(W, rows), pl.ds(T, depth)
    za, zb = pl.ds(T, half), pl.ds(T + half, depth - half)

    def load(source, buf, s, k):
        return pltpu.make_async_copy(
            source.at[s], grid.at[buf, s, xs, zs, :], load_sem.at[k, s]
        )

    for s in range(shots):
        load(now_hbm, 0, s, 0).start()
    scalars = [
        pltpu.make_async_copy(a, b, scalar_sem.at[i])
        for i, (a, b) in enumerate((
            (courant_hbm, courant), (cells_hbm, cells), (wavelet_hbm, wavelet),
        ))
    ]
    for copy in scalars:
        copy.start()
    load_class = pltpu.make_async_copy(class_hbm, klass, class_sem)
    load_class.start()
    for s in range(shots):
        load(before_hbm, 1, s, 1).start()

    pieces = [
        (0, xs, pl.ds(T, ZL), xs, pl.ds(T + depth, ZL)),
        (1, xs, pl.ds(T + depth - ZL, ZL), xs, pl.ds(T - ZL, ZL)),
        (2, pl.ds(W, W), za, pl.ds(W + rows, W), za),
        (3, pl.ds(rows, W), za, pl.ds(0, W), za),
    ]
    if relayed:
        pieces += [
            (2, pl.ds(W, W), zb, pl.ds(W + rows, W), zb),
            (3, pl.ds(rows, W), zb, pl.ds(0, W), zb),
        ]

    def halo(buf, s, k):
        d, sx, sz, dx, dz = pieces[k]
        return pltpu.make_async_remote_copy(
            src_ref=grid.at[buf, s, sx, sz, :],
            dst_ref=grid.at[buf, s, dx, dz, :],
            send_sem=send_sem.at[buf, s, k],
            recv_sem=recv_sem.at[buf, s, k],
            device_id=target(d),
            device_id_type=MESH,
        )

    def detour(r, buf, s, k):
        d, sx, sz, _, _ = pieces[k]
        return pltpu.make_async_remote_copy(
            src_ref=grid.at[buf, s, sx, sz, :],
            dst_ref=relay.at[r, s],
            send_sem=send_sem.at[buf, s, k],
            recv_sem=relay_sem.at[r, s],
            device_id=along(via[d]),
            device_id_type=MESH,
        )

    def forward(r, buf, s, k):
        d, _, _, dx, dz = pieces[k]
        return pltpu.make_async_remote_copy(
            src_ref=relay.at[r, s],
            dst_ref=grid.at[buf, s, dx, dz, :],
            send_sem=forward_sem.at[r, s],
            recv_sem=recv_sem.at[buf, s, k],
            device_id=along(serve_to[d]),
            device_id_type=MESH,
        )

    for d in range(4):
        _, _, _, dx, dz = pieces[d ^ 1]
        if d >= 2:
            dz = zs

        @pl.when(jnp.logical_not(has[d]))
        def _():
            for buf in range(2):
                def clear(s, c):
                    shape = (dx.size, dz.size, width)
                    grid[buf, s, dx, dz, :] = jnp.zeros(shape, jnp.float32)
                    return c
                lax.fori_loop(0, shots, clear, 0)

    meets = [(has[d], target(d)) for d in range(4)]
    if relayed:
        for d in (2, 3):
            step_back = -side + 1 if d == 2 else side - 1
            back = me - step_back - (1 if d == 2 else -1)
            meets.append((cross[d], along(via[d])))
            meets.append((serves[d], along(serve_from[d])))
            if side > 2:
                meets.append((serves[d], along(serve_to[d])))
                meets.append((cross[d], along(me + (side - 1 if d == 2 else 1 - side))))

    barrier = pltpu.get_barrier_semaphore()
    for there, device in meets:
        @pl.when(there)
        def _():
            pl.semaphore_signal(barrier, inc=1, device_id=device, device_id_type=MESH)
    peers = sum(there.astype(jnp.int32) for there, _ in meets)
    pl.semaphore_wait(barrier, peers)

    def each(ways, straight, around):
        for k in ways:
            d = pieces[k][0]
            if k < 4:
                pl.when(has[d])(lambda: straight(k))
            else:
                pl.when(cross[d])(lambda: around(k))
                pl.when(has[d] & jnp.logical_not(cross[d]))(lambda: straight(k))

    wide = (4, 5, 2, 3) if relayed else (2, 3)

    def send(r, buf, s, ways):
        each(ways, lambda k: halo(buf, s, k).start(), lambda k: detour(r, buf, s, k).start())

    def wait_sent(buf, s, ways):
        each(ways, lambda k: halo(buf, s, k).wait_send(),
             lambda k: detour(0, buf, s, k).wait_send())

    def wait_halo(buf, s, ways):
        for k in ways:
            pl.when(has[pieces[k][0] ^ 1])(lambda: halo(buf, s, k).wait_recv())

    def pass_on(r, s):
        if not relayed:
            return
        for k in (4, 5):
            @pl.when(serves[pieces[k][0]])
            def _():
                buf = r % 2 if isinstance(r, int) else lax.rem(r, 2)
                detour(r, buf, s, k).wait_recv()
                forward(r, buf, s, k).start()

    for s in range(shots):
        load(now_hbm, 0, s, 0).wait()
        send(0, 0, s, wide + (0, 1))

    for copy in scalars:
        copy.wait()
    z_index = place["depth"] * depth + lax.broadcasted_iota(jnp.int32, (depth, width), 0)
    total = depth * sizes["depth"]
    begin = jnp.full((depth, width), start[0], jnp.int32)
    ratio = (z_index - begin + 1).astype(jnp.float32) / (total - begin).astype(jnp.float32)
    damping = jnp.where(z_index >= begin, DAMPING * ratio * ratio, jnp.float32(0.0))
    inverse = 1.0 / (1.0 + damping)
    scale[0] = inverse
    scale[1] = 2.0 * inverse

    load_class.wait()

    def lookup(x, c):
        held = klass[x]
        value = jnp.zeros((depth, width), jnp.float32)
        for k in range(classes):
            value = jnp.where(held == k, courant[k], value)
        speed[x] = value * scale[0]
        return c

    lax.fori_loop(0, rows, lookup, 0)
    for s in range(shots):
        load(before_hbm, 1, s, 1).wait()

    lag = min(LAG, shots)
    for s in range(shots - lag):
        pass_on(0, s)

    lane = lax.broadcasted_iota(jnp.int32, (T, width), 1)
    low = [jnp.where(lane >= k, jnp.float32(COEFFS[k]), 0.0) for k in range(1, W + 1)]
    high = [jnp.where(lane < width - k, jnp.float32(COEFFS[k]), 0.0) for k in range(1, W + 1)]
    x_anchor = place["gx"] * rows

    def compute(t, s, buf, other, first, group, stride, count):
        lane_z = lax.broadcasted_iota(jnp.int32, (depth, width), 1)
        hit = (z_index == cells[s, 1]) & (lane_z == cells[s, 2])
        pulse = jnp.where(hit, wavelet[s, t] * scale[0], 0.0)
        cell_x = cells[s, 0] - x_anchor

        def block_of(x, j):
            z = T + j * T

            def at(dx, dz):
                return grid[buf, s, x + W + dx, pl.ds(z + dz, T), :]

            p = at(0, 0)
            lap = (3.0 * COEFFS[0]) * p
            for k in range(1, W + 1):
                pair = (at(k, 0) + at(-k, 0)) + (at(0, k) + at(0, -k))
                lap = lap + COEFFS[k] * pair
                lap = lap + (
                    low[k - 1] * pltpu.roll(p, k, 1)
                    + high[k - 1] * pltpu.roll(p, width - k, 1)
                )
            q = grid[other, s, x + W, pl.ds(z, T), :]
            block = pl.ds(j * T, T)
            nxt = scale[1, block, :] * (p - q) + q + speed[x, block, :] * lap
            amp = jnp.where(x == cell_x, jnp.float32(1.0), jnp.float32(0.0))
            return nxt + amp * pulse[j * T : (j + 1) * T]

        def row(g, c):
            begin = first + g * stride
            spots = [(begin + i, j) for i in range(group) for j in range(depth // T)]
            values = [block_of(x, j) for x, j in spots]
            for (x, j), value in zip(spots, values):
                grid[other, s, x + W, pl.ds(T + j * T, T), :] = value
            return c

        lax.fori_loop(0, count, row, 0)

    inner = rows - 2 * W
    group = math.gcd(inner, GROUP)

    def step(t, c):
        buf = lax.rem(t, 2)
        other = 1 - buf

        def shot(s, c):
            wait_halo(buf, s, (0, 1))
            pl.when(t >= 1)(lambda: wait_sent(other, s, (0, 1)))
            compute(t, s, buf, other, W, group, group, inner // group)
            wait_halo(buf, s, wide)
            pl.when(t >= 1)(lambda: wait_sent(other, s, wide))
            compute(t, s, buf, other, 0, W, rows - W, 2)

            @pl.when(t < iters - 1)
            def _():
                send(t + 1, other, s, wide + (0, 1))

            unit = t * shots + s + shots - lag
            r, u = unit // shots, lax.rem(unit, shots)
            pl.when(r < iters)(lambda: pass_on(r, u))
            return c

        return lax.fori_loop(0, shots, shot, c)

    lax.fori_loop(0, iters, step, 0)
    for s in range(shots):
        wait_sent(1 - iters % 2, s, wide + (0, 1))
    if relayed:
        for k in (4, 5):
            @pl.when(serves[pieces[k][0]])
            def _():
                def gone(i, c):
                    r = i // shots
                    forward(r, lax.rem(r, 2), lax.rem(i, shots), k).wait_send()
                    return c
                lax.fori_loop(0, iters * shots, gone, 0)


def put_out(iters, shots, rows, depth, grid, final_hbm, prior_hbm, out_sem):
    xs, zs = pl.ds(W, rows), pl.ds(T, depth)
    copies = [
        pltpu.make_async_copy(grid.at[buf, s, xs, zs, :], out.at[s], out_sem.at[k, s])
        for s in range(shots)
        for k, (buf, out) in enumerate(((iters % 2, final_hbm), (1 - iters % 2, prior_hbm)))
    ]
    for copy in copies:
        copy.start()
    for copy in copies:
        copy.wait()


def solution(mesh):
    sizes = {axis: mesh.shape[axis] for axis in ("depth", "gx")}
    side = math.isqrt(sizes["gx"])
    if side * side != sizes["gx"]:
        side = 0

    def local(now, before, class_map, courant, cells, wavelet, start):
        shots, rows, depth, width = now.shape
        iters = wavelet.shape[0]
        split = side if depth >= 2 * T else 0
        body = functools.partial(
            kernel, sizes, split, iters, shots, rows, depth, width, courant.shape[0]
        )
        whole = pl.BlockSpec(memory_space=pl.ANY)
        far = pl.BlockSpec(memory_space=pltpu.HBM)
        out = jax.ShapeDtypeStruct(now.shape, jnp.float32)
        half = max(T, depth // 2 // T * T)
        operands = [
            pltpu.with_memory_space_constraint(a, pltpu.HBM)
            for a in (now, before, class_map, courant, cells, wavelet.T)
        ]
        grid = pl.pallas_call(
            body,
            out_shape=pltpu.VMEM(
                (2, shots, rows + 2 * W, depth + 2 * T, width), jnp.float32
            ),
            in_specs=[far] * len(operands) + [pl.BlockSpec(memory_space=pltpu.SMEM)],
            out_specs=pl.BlockSpec(memory_space=pltpu.VMEM),
            scratch_shapes=[
                pltpu.SMEM(courant.shape, courant.dtype),
                pltpu.SMEM(cells.shape, cells.dtype),
                pltpu.SMEM(wavelet.shape[::-1], wavelet.dtype),
                pltpu.SemaphoreType.DMA((3,)),
                pltpu.VMEM((iters, shots, W, depth - half, width), jnp.float32),
                pltpu.VMEM((rows, depth, width), jnp.float32),
                pltpu.VMEM((2, depth, width), jnp.float32),
                pltpu.VMEM((rows, depth, width), jnp.int32),
                pltpu.SemaphoreType.DMA((2, shots)),
                pltpu.SemaphoreType.DMA,
                pltpu.SemaphoreType.DMA((2, shots, 6)),
                pltpu.SemaphoreType.DMA((2, shots, 6)),
                pltpu.SemaphoreType.DMA((iters, shots)),
                pltpu.SemaphoreType.DMA((iters, shots)),
            ],
            compiler_params=pltpu.CompilerParams(
                collective_id=0, has_side_effects=True, vmem_limit_bytes=16 * 1024 * 1024
            ),
            name="wave",
        )(*operands, start)
        grid = pltpu.with_memory_space_constraint(grid, pltpu.VMEM)
        return pl.pallas_call(
            functools.partial(put_out, iters, shots, rows, depth),
            out_shape=(out, out),
            in_specs=[whole],
            out_specs=(whole, whole),
            scratch_shapes=[pltpu.SemaphoreType.DMA((2, shots))],
            compiler_params=pltpu.CompilerParams(vmem_limit_bytes=1024 * 1024),
            name="put_out",
        )(grid)

    placed = P(None, "gx", "depth", None)
    return jax.shard_map(
        local,
        mesh=mesh,
        in_specs=(placed, placed, P("gx", "depth", None), P(), P(), P(), P()),
        out_specs=(placed, placed),
        check_vma=False,
    )
```

```python
import functools
import math

import jax
import jax.numpy as jnp
from jax import lax
from jax.experimental import pallas as pl
from jax.experimental.pallas import tpu as pltpu
from jax.sharding import PartitionSpec as P

COEFFS = (-205.0 / 72.0, 8.0 / 5.0, -1.0 / 5.0, 8.0 / 315.0, -1.0 / 560.0)
DAMPING = 0.3
GROUP = 8
W = 4
T = 8
LAG = 2
ZL = W
DIRS = (("depth", -1), ("depth", 1), ("gx", -1), ("gx", 1))
MESH = pl.DeviceIdType.MESH


def kernel(
    sizes, side, iters, shots, rows, depth, width, classes,
    now_hbm, before_hbm, class_hbm, courant_hbm, cells_hbm, wavelet_hbm, start,
    grid,
    courant, cells, wavelet, scalar_sem,
    relay, speed, scale, klass, load_sem, class_sem,
    send_sem, recv_sem, relay_sem, forward_sem,
):
    place = {axis: lax.axis_index(axis) for axis in ("depth", "gx")}
    me = place["gx"]
    lanes = sizes["gx"]
    has = []
    for axis, delta in DIRS:
        has.append(place[axis] > 0 if delta < 0 else place[axis] < sizes[axis] - 1)

    def along(g):
        return (place["depth"], g)

    def target(d):
        axis, delta = DIRS[d]
        there = dict(place)
        there[axis] = place[axis] + delta
        return (there["depth"], there["gx"])

    relayed = side > 1
    if relayed:
        column = lax.rem(me, side)
        cross = {2: has[2] & (column == 0), 3: has[3] & (column == side - 1)}
        via = {2: me - side, 3: me + side}
        serves = {
            2: (column == 0) & (me + side < lanes),
            3: (column == side - 1) & (me - side >= 0),
        }
        serve_from = {2: me + side, 3: me - side}
        serve_to = {2: me + side - 1, 3: me - side + 1}

    meets = [(has[d], target(d)) for d in range(4)]
    if relayed:
        for d in (2, 3):
            step_back = -side + 1 if d == 2 else side - 1
            back = me - step_back - (1 if d == 2 else -1)
            meets.append((cross[d], along(via[d])))
            meets.append((serves[d], along(serve_from[d])))
            if side > 2:
                meets.append((serves[d], along(serve_to[d])))
                meets.append((cross[d], along(me + (side - 1 if d == 2 else 1 - side))))

    barrier = pltpu.get_barrier_semaphore()
    for there, device in meets:
        @pl.when(there)
        def _():
            pl.semaphore_signal(barrier, inc=1, device_id=device, device_id_type=MESH)

    half = max(T, depth // 2 // T * T) if relayed else depth

    xs, zs = pl.ds(W, rows), pl.ds(T, depth)
    za, zb = pl.ds(T, half), pl.ds(T + half, depth - half)

    def load(source, buf, s, k):
        return pltpu.make_async_copy(
            source.at[s], grid.at[buf, s, xs, zs, :], load_sem.at[k, s]
        )

    for s in range(shots):
        load(now_hbm, 0, s, 0).start()
    scalars = [
        pltpu.make_async_copy(a, b, scalar_sem.at[i])
        for i, (a, b) in enumerate((
            (courant_hbm, courant), (cells_hbm, cells), (wavelet_hbm, wavelet),
        ))
    ]
    for copy in scalars:
        copy.start()
    load_class = pltpu.make_async_copy(class_hbm, klass, class_sem)

    pieces = [
        (0, xs, pl.ds(T, ZL), xs, pl.ds(T + depth, ZL)),
        (1, xs, pl.ds(T + depth - ZL, ZL), xs, pl.ds(T - ZL, ZL)),
        (2, pl.ds(W, W), za, pl.ds(W + rows, W), za),
        (3, pl.ds(rows, W), za, pl.ds(0, W), za),
    ]
    if relayed:
        pieces += [
            (2, pl.ds(W, W), zb, pl.ds(W + rows, W), zb),
            (3, pl.ds(rows, W), zb, pl.ds(0, W), zb),
            (2, pl.ds(W, W), zs, pl.ds(W + rows, W), zs),
            (3, pl.ds(rows, W), zs, pl.ds(0, W), zs),
        ]

    def halo(buf, s, k):
        d, sx, sz, dx, dz = pieces[k]
        return pltpu.make_async_remote_copy(
            src_ref=grid.at[buf, s, sx, sz, :],
            dst_ref=grid.at[buf, s, dx, dz, :],
            send_sem=send_sem.at[buf, s, k],
            recv_sem=recv_sem.at[buf, s, k],
            device_id=target(d),
            device_id_type=MESH,
        )

    def detour(r, buf, s, k):
        d, sx, sz, _, _ = pieces[k]
        return pltpu.make_async_remote_copy(
            src_ref=grid.at[buf, s, sx, sz, :],
            dst_ref=relay.at[r, s],
            send_sem=send_sem.at[buf, s, k],
            recv_sem=relay_sem.at[r, s],
            device_id=along(via[d]),
            device_id_type=MESH,
        )

    def forward(r, buf, s, k):
        d, _, _, dx, dz = pieces[k]
        return pltpu.make_async_remote_copy(
            src_ref=relay.at[r, s],
            dst_ref=grid.at[buf, s, dx, dz, :],
            send_sem=forward_sem.at[r, s],
            recv_sem=recv_sem.at[buf, s, k],
            device_id=along(serve_to[d]),
            device_id_type=MESH,
        )

    for d in range(4):
        _, _, _, dx, dz = pieces[d ^ 1]
        if d >= 2:
            dz = zs

        @pl.when(jnp.logical_not(has[d]))
        def _():
            for buf in range(2):
                def clear(s, c):
                    shape = (dx.size, dz.size, width)
                    grid[buf, s, dx, dz, :] = jnp.zeros(shape, jnp.float32)
                    return c
                lax.fori_loop(0, shots, clear, 0)

    peers = sum(there.astype(jnp.int32) for there, _ in meets)
    pl.semaphore_wait(barrier, peers)

    def each(ways, straight, around):
        for d in ways:
            if d < 2 or not relayed:
                pl.when(has[d])(lambda: straight(d))
                continue

            @pl.when(cross[d])
            def _():
                around(d + 2)
                straight(d)

            pl.when(has[d] & jnp.logical_not(cross[d]))(lambda: straight(d + 4))

    wide = (2, 3)

    def send(r, buf, s, ways):
        each(ways, lambda k: halo(buf, s, k).start(), lambda k: detour(r, buf, s, k).start())

    def send_around(r, buf, s):
        if relayed:
            for d in wide:
                pl.when(cross[d])(lambda: detour(r, buf, s, d + 2).start())

    def send_straight(r, buf, s):
        each(wide, lambda k: halo(buf, s, k).start(), lambda k: None)

    def wait_sent(buf, s, ways):
        each(ways, lambda k: halo(buf, s, k).wait_send(),
             lambda k: detour(0, buf, s, k).wait_send())

    def wait_halo(buf, s, ways):
        for d in ways:
            if d < 2 or not relayed:
                pl.when(has[d ^ 1])(lambda: halo(buf, s, d).wait_recv())
                continue

            @pl.when(cross[d ^ 1])
            def _():
                halo(buf, s, d).wait_recv()
                halo(buf, s, d + 2).wait_recv()

            plain = has[d ^ 1] & jnp.logical_not(cross[d ^ 1])
            pl.when(plain)(lambda: halo(buf, s, d + 4).wait_recv())

    def pass_on(r, s):
        if not relayed:
            return
        for k in (4, 5):
            @pl.when(serves[pieces[k][0]])
            def _():
                buf = r % 2 if isinstance(r, int) else lax.rem(r, 2)
                detour(r, buf, s, k).wait_recv()
                forward(r, buf, s, k).start()

    lag = min(LAG, shots)
    early = min(lag, shots)
    for s in range(early):
        load(now_hbm, 0, s, 0).wait()
        send(0, 0, s, wide)
    for s in range(early, shots):
        load(now_hbm, 0, s, 0).wait()
        send_around(0, 0, s)
    for s in range(shots):
        send(0, 0, s, (0, 1))
    load_class.start()
    for s in range(shots):
        load(before_hbm, 1, s, 1).start()

    for copy in scalars:
        copy.wait()
    z_index = place["depth"] * depth + lax.broadcasted_iota(jnp.int32, (depth, width), 0)
    total = depth * sizes["depth"]
    begin = jnp.full((depth, width), start[0], jnp.int32)
    ratio = (z_index - begin + 1).astype(jnp.float32) / (total - begin).astype(jnp.float32)
    damping = jnp.where(z_index >= begin, DAMPING * ratio * ratio, jnp.float32(0.0))
    inverse = 1.0 / (1.0 + damping)
    scale[0] = inverse
    scale[1] = 2.0 * inverse

    load_class.wait()

    def lookup(x, c):
        held = klass[x]
        value = jnp.zeros((depth, width), jnp.float32)
        for k in range(classes):
            value = jnp.where(held == k, courant[k], value)
        speed[x] = value * scale[0]
        return c

    lax.fori_loop(0, rows, lookup, 0)
    for s in range(shots):
        load(before_hbm, 1, s, 1).wait()

    for s in range(early, shots):
        pass_on(0, s - early)
        send_straight(0, 0, s)

    lane = lax.broadcasted_iota(jnp.int32, (T, width), 1)
    low = [jnp.where(lane >= k, jnp.float32(COEFFS[k]), 0.0) for k in range(1, W + 1)]
    high = [jnp.where(lane < width - k, jnp.float32(COEFFS[k]), 0.0) for k in range(1, W + 1)]
    x_anchor = place["gx"] * rows

    group = math.gcd(rows, GROUP)

    def compute(t, s, buf, other):
        lane_z = lax.broadcasted_iota(jnp.int32, (depth, width), 1)
        hit = (z_index == cells[s, 1]) & (lane_z == cells[s, 2])
        pulse = jnp.where(hit, wavelet[s, t] * scale[0], 0.0)
        cell_x = cells[s, 0] - x_anchor

        def block_of(x, j, above, below):
            z = T + j * T

            def at(dx, dz):
                return grid[buf, s, x + W + dx, pl.ds(z + dz, T), :]

            p = at(0, 0)
            lap = (3.0 * COEFFS[0]) * p
            for k in range(1, W + 1):
                pair = at(0, k) + at(0, -k)
                if k <= above:
                    pair = pair + at(-k, 0)
                if k <= below:
                    pair = pair + at(k, 0)
                lap = lap + COEFFS[k] * pair
                lap = lap + (
                    low[k - 1] * pltpu.roll(p, k, 1)
                    + high[k - 1] * pltpu.roll(p, width - k, 1)
                )
            q = grid[other, s, x + W, pl.ds(z, T), :]
            block = pl.ds(j * T, T)
            nxt = scale[1, block, :] * (p - q) + q + speed[x, block, :] * lap
            amp = jnp.where(x == cell_x, jnp.float32(1.0), jnp.float32(0.0))
            return nxt + amp * pulse[j * T : (j + 1) * T]

        def run(begin, top, bottom):
            spots = [(i, j) for i in range(group) for j in range(depth // T)]
            values = [
                block_of(begin + i, j, i if top else W, group - 1 - i if bottom else W)
                for i, j in spots
            ]
            for (i, j), value in zip(spots, values):
                grid[other, s, begin + i + W, pl.ds(T + j * T, T), :] = value

        count = rows // group
        run(0, True, count == 1)
        if count > 1:
            run(rows - group, False, True)

        def row(g, c):
            run(g * group, False, False)
            return c

        lax.fori_loop(1, count - 1, row, 0)

    def complete(s, buf, other):
        for j in range(depth // T):
            z = pl.ds(T + j * T, T)
            block = pl.ds(j * T, T)
            ahead = [grid[buf, s, W - 1 - k, z, :] for k in range(W)]
            after = [grid[buf, s, W + rows + k, z, :] for k in range(W)]
            for i in range(W):
                for x, beyond in ((i, ahead), (rows - 1 - i, after)):
                    lap = COEFFS[i + 1] * beyond[0]
                    for k in range(1, W - i):
                        lap = lap + COEFFS[i + 1 + k] * beyond[k]
                    partial = grid[other, s, x + W, z, :]
                    grid[other, s, x + W, z, :] = partial + speed[x, block, :] * lap

    def step(t, c):
        buf = lax.rem(t, 2)
        other = 1 - buf

        def shot(s, c):
            wait_halo(buf, s, (0, 1))
            pl.when(t >= 1)(lambda: wait_sent(other, s, (0, 1) + wide))
            compute(t, s, buf, other)

            unit = t * shots + s + shots - lag
            r, u = unit // shots, lax.rem(unit, shots)
            pl.when(r < iters)(lambda: pass_on(r, u))

            wait_halo(buf, s, wide)
            complete(s, buf, other)

            @pl.when(t < iters - 1)
            def _():
                send(t + 1, other, s, wide + (0, 1))

            return c

        return lax.fori_loop(0, shots, shot, c)

    lax.fori_loop(0, iters, step, 0)
    for s in range(shots):
        wait_sent(1 - iters % 2, s, wide + (0, 1))
    if relayed:
        for k in (4, 5):
            @pl.when(serves[pieces[k][0]])
            def _():
                def gone(i, c):
                    r = i // shots
                    forward(r, lax.rem(r, 2), lax.rem(i, shots), k).wait_send()
                    return c
                lax.fori_loop(0, iters * shots, gone, 0)


def put_out(iters, shots, rows, depth, grid, final_hbm, prior_hbm, out_sem):
    xs, zs = pl.ds(W, rows), pl.ds(T, depth)
    copies = [
        pltpu.make_async_copy(grid.at[buf, s, xs, zs, :], out.at[s], out_sem.at[k, s])
        for s in range(shots)
        for k, (buf, out) in enumerate(((iters % 2, final_hbm), (1 - iters % 2, prior_hbm)))
    ]
    for copy in copies:
        copy.start()
    for copy in copies:
        copy.wait()


def solution(mesh):
    sizes = {axis: mesh.shape[axis] for axis in ("depth", "gx")}
    side = math.isqrt(sizes["gx"])
    if side * side != sizes["gx"]:
        side = 0

    def local(now, before, class_map, courant, cells, wavelet, start):
        shots, rows, depth, width = now.shape
        iters = wavelet.shape[0]
        split = side if depth >= 2 * T else 0
        body = functools.partial(
            kernel, sizes, split, iters, shots, rows, depth, width, courant.shape[0]
        )
        whole = pl.BlockSpec(memory_space=pl.ANY)
        far = pl.BlockSpec(memory_space=pltpu.HBM)
        out = jax.ShapeDtypeStruct(now.shape, jnp.float32)
        half = max(T, depth // 2 // T * T)
        operands = [
            pltpu.with_memory_space_constraint(a, pltpu.HBM)
            for a in (now, before, class_map, courant, cells, wavelet.T)
        ]
        grid = pl.pallas_call(
            body,
            out_shape=pltpu.VMEM(
                (2, shots, rows + 2 * W, depth + 2 * T, width), jnp.float32
            ),
            in_specs=[far] * len(operands) + [pl.BlockSpec(memory_space=pltpu.SMEM)],
            out_specs=pl.BlockSpec(memory_space=pltpu.VMEM),
            scratch_shapes=[
                pltpu.SMEM(courant.shape, courant.dtype),
                pltpu.SMEM(cells.shape, cells.dtype),
                pltpu.SMEM(wavelet.shape[::-1], wavelet.dtype),
                pltpu.SemaphoreType.DMA((3,)),
                pltpu.VMEM((iters, shots, W, depth - half, width), jnp.float32),
                pltpu.VMEM((rows, depth, width), jnp.float32),
                pltpu.VMEM((2, depth, width), jnp.float32),
                pltpu.VMEM((rows, depth, width), jnp.int32),
                pltpu.SemaphoreType.DMA((2, shots)),
                pltpu.SemaphoreType.DMA,
                pltpu.SemaphoreType.DMA((2, shots, 8)),
                pltpu.SemaphoreType.DMA((2, shots, 8)),
                pltpu.SemaphoreType.DMA((iters, shots)),
                pltpu.SemaphoreType.DMA((iters, shots)),
            ],
            compiler_params=pltpu.CompilerParams(
                collective_id=0, has_side_effects=True, vmem_limit_bytes=16 * 1024 * 1024
            ),
            name="wave",
        )(*operands, start)
        grid = pltpu.with_memory_space_constraint(grid, pltpu.VMEM)
        return pl.pallas_call(
            functools.partial(put_out, iters, shots, rows, depth),
            out_shape=(out, out),
            in_specs=[whole],
            out_specs=(whole, whole),
            scratch_shapes=[pltpu.SemaphoreType.DMA((2, shots))],
            compiler_params=pltpu.CompilerParams(vmem_limit_bytes=1024 * 1024),
            name="put_out",
        )(grid)

    placed = P(None, "gx", "depth", None)
    return jax.shard_map(
        local,
        mesh=mesh,
        in_specs=(placed, placed, P("gx", "depth", None), P(), P(), P(), P()),
        out_specs=(placed, placed),
        check_vma=False,
    )
```

```python
import functools
import math

import jax
import jax.numpy as jnp
from jax import lax
from jax.experimental import pallas as pl
from jax.experimental.pallas import tpu as pltpu
from jax.sharding import PartitionSpec as P

COEFFS = (-205.0 / 72.0, 8.0 / 5.0, -1.0 / 5.0, 8.0 / 315.0, -1.0 / 560.0)
DAMPING = 0.3
GROUP = 8
W = 4
T = 8
LAG = 2
ZL = W
DIRS = (("depth", -1), ("depth", 1), ("gx", -1), ("gx", 1))
MESH = pl.DeviceIdType.MESH


def kernel(
    sizes, side, iters, shots, rows, depth, width, classes,
    now_hbm, before_hbm, class_hbm, courant_hbm, cells_hbm, wavelet_hbm, start,
    grid,
    courant, cells, wavelet, scalar_sem,
    relay, speed, scale, klass, load_sem, class_sem,
    send_sem, recv_sem, relay_sem, forward_sem,
):
    place = {axis: lax.axis_index(axis) for axis in ("depth", "gx")}
    me = place["gx"]
    lanes = sizes["gx"]
    has = []
    for axis, delta in DIRS:
        has.append(place[axis] > 0 if delta < 0 else place[axis] < sizes[axis] - 1)

    def along(g):
        return (place["depth"], g)

    def target(d):
        axis, delta = DIRS[d]
        there = dict(place)
        there[axis] = place[axis] + delta
        return (there["depth"], there["gx"])

    relayed = side > 1
    if relayed:
        column = lax.rem(me, side)
        cross = {2: has[2] & (column == 0), 3: has[3] & (column == side - 1)}
        via = {2: me - side, 3: me + side}
        serves = {
            2: (column == 0) & (me + side < lanes),
            3: (column == side - 1) & (me - side >= 0),
        }
        serve_from = {2: me + side, 3: me - side}
        serve_to = {2: me + side - 1, 3: me - side + 1}

    meets = [(has[d], target(d)) for d in range(4)]
    if relayed:
        for d in (2, 3):
            step_back = -side + 1 if d == 2 else side - 1
            back = me - step_back - (1 if d == 2 else -1)
            meets.append((cross[d], along(via[d])))
            meets.append((serves[d], along(serve_from[d])))
            if side > 2:
                meets.append((serves[d], along(serve_to[d])))
                meets.append((cross[d], along(me + (side - 1 if d == 2 else 1 - side))))

    barrier = pltpu.get_barrier_semaphore()
    for there, device in meets:
        @pl.when(there)
        def _():
            pl.semaphore_signal(barrier, inc=1, device_id=device, device_id_type=MESH)

    half = max(T, depth // 2 // T * T) if relayed else depth

    xs, zs = pl.ds(W, rows), pl.ds(T, depth)
    za, zb = pl.ds(T, half), pl.ds(T + half, depth - half)

    def load(source, buf, s, k):
        return pltpu.make_async_copy(
            source.at[s], grid.at[buf, s, xs, zs, :], load_sem.at[k, s]
        )

    def passed(r, s):
        if relayed:
            for d in wide:
                pl.when(serves[d] & bends(r, s))(lambda: forward(r, lax.rem(r, 2), s, d + 2).wait_send())

    for s in range(shots):
        load(now_hbm, 0, s, 0).start()
    scalars = [
        pltpu.make_async_copy(a, b, scalar_sem.at[i])
        for i, (a, b) in enumerate((
            (courant_hbm, courant), (cells_hbm, cells), (wavelet_hbm, wavelet),
        ))
    ]
    for copy in scalars:
        copy.start()
    load_class = pltpu.make_async_copy(class_hbm, klass, class_sem)

    pieces = [
        (0, xs, pl.ds(T, ZL), xs, pl.ds(T + depth, ZL)),
        (1, xs, pl.ds(T + depth - ZL, ZL), xs, pl.ds(T - ZL, ZL)),
        (2, pl.ds(W, W), za, pl.ds(W + rows, W), za),
        (3, pl.ds(rows, W), za, pl.ds(0, W), za),
    ]
    if relayed:
        pieces += [
            (2, pl.ds(W, W), zb, pl.ds(W + rows, W), zb),
            (3, pl.ds(rows, W), zb, pl.ds(0, W), zb),
            (2, pl.ds(W, W), zs, pl.ds(W + rows, W), zs),
            (3, pl.ds(rows, W), zs, pl.ds(0, W), zs),
        ]

    def halo(buf, s, k):
        d, sx, sz, dx, dz = pieces[k]
        return pltpu.make_async_remote_copy(
            src_ref=grid.at[buf, s, sx, sz, :],
            dst_ref=grid.at[buf, s, dx, dz, :],
            send_sem=send_sem.at[buf, s, k],
            recv_sem=recv_sem.at[buf, s, k],
            device_id=target(d),
            device_id_type=MESH,
        )

    def detour(r, buf, s, k):
        d, sx, sz, _, _ = pieces[k]
        return pltpu.make_async_remote_copy(
            src_ref=grid.at[buf, s, sx, sz, :],
            dst_ref=relay.at[r, s],
            send_sem=send_sem.at[buf, s, k],
            recv_sem=relay_sem.at[r, s],
            device_id=along(via[d]),
            device_id_type=MESH,
        )

    def forward(r, buf, s, k):
        d, _, _, dx, dz = pieces[k]
        return pltpu.make_async_remote_copy(
            src_ref=relay.at[r, s],
            dst_ref=grid.at[buf, s, dx, dz, :],
            send_sem=forward_sem.at[r, s],
            recv_sem=recv_sem.at[buf, s, k],
            device_id=along(serve_to[d]),
            device_id_type=MESH,
        )

    for d in range(4):
        _, _, _, dx, dz = pieces[d ^ 1]
        if d >= 2:
            dz = zs

        @pl.when(jnp.logical_not(has[d]))
        def _():
            for buf in range(2):
                def clear(s, c):
                    shape = (dx.size, dz.size, width)
                    grid[buf, s, dx, dz, :] = jnp.zeros(shape, jnp.float32)
                    return c
                lax.fori_loop(0, shots, clear, 0)

    peers = sum(there.astype(jnp.int32) for there, _ in meets)
    pl.semaphore_wait(barrier, peers)

    def bends(r, s):
        last = (r == iters - 1) & (s == shots - 1)
        return jnp.logical_not(last)

    def each(ways, straight, around, bend=True):
        for d in ways:
            if d < 2 or not relayed:
                pl.when(has[d])(lambda: straight(d))
                continue

            @pl.when(cross[d] & bend)
            def _():
                around(d + 2)
                straight(d)

            pl.when(has[d] & jnp.logical_not(cross[d] & bend))(lambda: straight(d + 4))

    wide = (2, 3)

    def send(r, buf, s, ways):
        each(ways, lambda k: halo(buf, s, k).start(), lambda k: detour(r, buf, s, k).start(),
             bends(r, s))

    def send_around(r, buf, s):
        if relayed:
            for d in wide:
                pl.when(cross[d])(lambda: detour(r, buf, s, d + 2).start())

    def send_straight(r, buf, s):
        each(wide, lambda k: halo(buf, s, k).start(), lambda k: None)

    def wait_sent(r, buf, s, ways):
        each(ways, lambda k: halo(buf, s, k).wait_send(),
             lambda k: detour(0, buf, s, k).wait_send(), bends(r, s))

    def wait_halo(r, buf, s, ways):
        for d in ways:
            if d < 2 or not relayed:
                pl.when(has[d ^ 1])(lambda: halo(buf, s, d).wait_recv())
                continue

            bend = bends(r, s)

            @pl.when(cross[d ^ 1] & bend)
            def _():
                halo(buf, s, d).wait_recv()
                halo(buf, s, d + 2).wait_recv()

            plain = has[d ^ 1] & jnp.logical_not(cross[d ^ 1] & bend)
            pl.when(plain)(lambda: halo(buf, s, d + 4).wait_recv())

    def pass_on(r, s):
        if not relayed:
            return
        for k in (4, 5):
            @pl.when(serves[pieces[k][0]] & bends(r, s))
            def _():
                buf = r % 2 if isinstance(r, int) else lax.rem(r, 2)
                detour(r, buf, s, k).wait_recv()
                forward(r, buf, s, k).start()

    lag = min(LAG, shots)
    early = min(lag, shots)
    for s in range(early):
        load(now_hbm, 0, s, 0).wait()
        send(0, 0, s, wide)
    for s in range(early, shots):
        load(now_hbm, 0, s, 0).wait()
        send_around(0, 0, s)
    for s in range(shots):
        send(0, 0, s, (0, 1))
    load_class.start()
    for s in range(shots):
        load(before_hbm, 1, s, 1).start()

    for copy in scalars:
        copy.wait()
    z_index = place["depth"] * depth + lax.broadcasted_iota(jnp.int32, (depth, width), 0)
    total = depth * sizes["depth"]
    begin = jnp.full((depth, width), start[0], jnp.int32)
    ratio = (z_index - begin + 1).astype(jnp.float32) / (total - begin).astype(jnp.float32)
    damping = jnp.where(z_index >= begin, DAMPING * ratio * ratio, jnp.float32(0.0))
    inverse = 1.0 / (1.0 + damping)
    scale[0] = inverse
    scale[1] = 2.0 * inverse

    load_class.wait()

    def lookup(x, c):
        held = klass[x]
        value = jnp.zeros((depth, width), jnp.float32)
        for k in range(classes):
            value = jnp.where(held == k, courant[k], value)
        speed[x] = value * scale[0]
        return c

    lax.fori_loop(0, rows, lookup, 0)
    for s in range(shots):
        load(before_hbm, 1, s, 1).wait()

    for s in range(early, shots):
        pass_on(0, s - early)
        send_straight(0, 0, s)

    lane = lax.broadcasted_iota(jnp.int32, (T, width), 1)
    low = [jnp.where(lane >= k, jnp.float32(COEFFS[k]), 0.0) for k in range(1, W + 1)]
    high = [jnp.where(lane < width - k, jnp.float32(COEFFS[k]), 0.0) for k in range(1, W + 1)]
    x_anchor = place["gx"] * rows

    group = math.gcd(rows, GROUP)

    def compute(t, s, buf, other):
        lane_z = lax.broadcasted_iota(jnp.int32, (depth, width), 1)
        hit = (z_index == cells[s, 1]) & (lane_z == cells[s, 2])
        pulse = jnp.where(hit, wavelet[s, t] * scale[0], 0.0)
        cell_x = cells[s, 0] - x_anchor

        def block_of(x, j, above, below):
            z = T + j * T

            def at(dx, dz):
                return grid[buf, s, x + W + dx, pl.ds(z + dz, T), :]

            p = at(0, 0)
            lap = (3.0 * COEFFS[0]) * p
            for k in range(1, W + 1):
                pair = at(0, k) + at(0, -k)
                if k <= above:
                    pair = pair + at(-k, 0)
                if k <= below:
                    pair = pair + at(k, 0)
                lap = lap + COEFFS[k] * pair
                lap = lap + (
                    low[k - 1] * pltpu.roll(p, k, 1)
                    + high[k - 1] * pltpu.roll(p, width - k, 1)
                )
            q = grid[other, s, x + W, pl.ds(z, T), :]
            block = pl.ds(j * T, T)
            nxt = scale[1, block, :] * (p - q) + q + speed[x, block, :] * lap
            amp = jnp.where(x == cell_x, jnp.float32(1.0), jnp.float32(0.0))
            return nxt + amp * pulse[j * T : (j + 1) * T]

        def run(begin, top, bottom):
            spots = [(i, j) for i in range(group) for j in range(depth // T)]
            values = [
                block_of(begin + i, j, i if top else W, group - 1 - i if bottom else W)
                for i, j in spots
            ]
            for (i, j), value in zip(spots, values):
                grid[other, s, begin + i + W, pl.ds(T + j * T, T), :] = value

        count = rows // group
        run(0, True, count == 1)
        if count > 1:
            run(rows - group, False, True)

        def row(g, c):
            run(g * group, False, False)
            return c

        lax.fori_loop(1, count - 1, row, 0)

    def complete(s, buf, other):
        for j in range(depth // T):
            z = pl.ds(T + j * T, T)
            block = pl.ds(j * T, T)
            ahead = [grid[buf, s, W - 1 - k, z, :] for k in range(W)]
            after = [grid[buf, s, W + rows + k, z, :] for k in range(W)]
            for i in range(W):
                for x, beyond in ((i, ahead), (rows - 1 - i, after)):
                    lap = COEFFS[i + 1] * beyond[0]
                    for k in range(1, W - i):
                        lap = lap + COEFFS[i + 1 + k] * beyond[k]
                    partial = grid[other, s, x + W, z, :]
                    grid[other, s, x + W, z, :] = partial + speed[x, block, :] * lap

    def step(t, c):
        buf = lax.rem(t, 2)
        other = 1 - buf

        def shot(s, c):
            wait_halo(t, buf, s, (0, 1))
            compute(t, s, buf, other)
            wait_sent(t, buf, s, (0, 1) + wide)
            passed(t, s)

            unit = t * shots + s + shots - lag
            r, u = unit // shots, lax.rem(unit, shots)
            pl.when(r < iters)(lambda: pass_on(r, u))

            wait_halo(t, buf, s, wide)
            complete(s, buf, other)

            @pl.when(t < iters - 1)
            def _():
                send(t + 1, other, s, wide + (0, 1))

            return c

        return lax.fori_loop(0, shots, shot, c)

    lax.fori_loop(0, iters, step, 0)


def put_out(iters, shots, rows, depth, grid, final_hbm, prior_hbm, out_sem):
    xs, zs = pl.ds(W, rows), pl.ds(T, depth)
    copies = [
        pltpu.make_async_copy(grid.at[buf, s, xs, zs, :], out.at[s], out_sem.at[k, s])
        for s in range(shots)
        for k, (buf, out) in enumerate(((iters % 2, final_hbm), (1 - iters % 2, prior_hbm)))
    ]
    for copy in copies:
        copy.start()
    for copy in copies:
        copy.wait()


def solution(mesh):
    sizes = {axis: mesh.shape[axis] for axis in ("depth", "gx")}
    side = math.isqrt(sizes["gx"])
    if side * side != sizes["gx"]:
        side = 0

    def local(now, before, class_map, courant, cells, wavelet, start):
        shots, rows, depth, width = now.shape
        iters = wavelet.shape[0]
        split = side if depth >= 2 * T else 0
        body = functools.partial(
            kernel, sizes, split, iters, shots, rows, depth, width, courant.shape[0]
        )
        whole = pl.BlockSpec(memory_space=pl.ANY)
        far = pl.BlockSpec(memory_space=pltpu.HBM)
        out = jax.ShapeDtypeStruct(now.shape, jnp.float32)
        half = max(T, depth // 2 // T * T)
        operands = [
            pltpu.with_memory_space_constraint(a, pltpu.HBM)
            for a in (now, before, class_map, courant, cells, wavelet.T)
        ]
        grid = pl.pallas_call(
            body,
            out_shape=pltpu.VMEM(
                (2, shots, rows + 2 * W, depth + 2 * T, width), jnp.float32
            ),
            in_specs=[far] * len(operands) + [pl.BlockSpec(memory_space=pltpu.SMEM)],
            out_specs=pl.BlockSpec(memory_space=pltpu.VMEM),
            scratch_shapes=[
                pltpu.SMEM(courant.shape, courant.dtype),
                pltpu.SMEM(cells.shape, cells.dtype),
                pltpu.SMEM(wavelet.shape[::-1], wavelet.dtype),
                pltpu.SemaphoreType.DMA((3,)),
                pltpu.VMEM((iters, shots, W, depth - half, width), jnp.float32),
                pltpu.VMEM((rows, depth, width), jnp.float32),
                pltpu.VMEM((2, depth, width), jnp.float32),
                pltpu.VMEM((rows, depth, width), jnp.int32),
                pltpu.SemaphoreType.DMA((2, shots)),
                pltpu.SemaphoreType.DMA,
                pltpu.SemaphoreType.DMA((2, shots, 8)),
                pltpu.SemaphoreType.DMA((2, shots, 8)),
                pltpu.SemaphoreType.DMA((iters, shots)),
                pltpu.SemaphoreType.DMA((iters, shots)),
            ],
            compiler_params=pltpu.CompilerParams(
                collective_id=0, has_side_effects=True, vmem_limit_bytes=16 * 1024 * 1024
            ),
            name="wave",
        )(*operands, start)
        grid = pltpu.with_memory_space_constraint(grid, pltpu.VMEM)
        return pl.pallas_call(
            functools.partial(put_out, iters, shots, rows, depth),
            out_shape=(out, out),
            in_specs=[whole],
            out_specs=(whole, whole),
            scratch_shapes=[pltpu.SemaphoreType.DMA((2, shots))],
            compiler_params=pltpu.CompilerParams(vmem_limit_bytes=1024 * 1024),
            name="put_out",
        )(grid)

    placed = P(None, "gx", "depth", None)
    return jax.shard_map(
        local,
        mesh=mesh,
        in_specs=(placed, placed, P("gx", "depth", None), P(), P(), P(), P()),
        out_specs=(placed, placed),
        check_vma=False,
    )
```

```python
import functools
import math

import jax
import jax.numpy as jnp
from jax import lax
from jax.experimental import pallas as pl
from jax.experimental.pallas import tpu as pltpu
from jax.sharding import PartitionSpec as P

COEFFS = (-205.0 / 72.0, 8.0 / 5.0, -1.0 / 5.0, 8.0 / 315.0, -1.0 / 560.0)
DAMPING = 0.3
GROUP = 8
W = 4
T = 8
LAG = 2
ZL = W
DIRS = (("depth", -1), ("depth", 1), ("gx", -1), ("gx", 1))
MESH = pl.DeviceIdType.MESH


def kernel(
    sizes, side, iters, shots, rows, depth, width, classes,
    now_hbm, before_hbm, class_hbm, courant_hbm, cells_hbm, wavelet_hbm, start_hbm,
    grid,
    courant, cells, wavelet, start, scalar_sem,
    relay, speed, scale, klass, load_sem, class_sem,
    send_sem, recv_sem, relay_sem, forward_sem,
):
    place = {axis: lax.axis_index(axis) for axis in ("depth", "gx")}
    me = place["gx"]
    lanes = sizes["gx"]
    has = []
    for axis, delta in DIRS:
        has.append(place[axis] > 0 if delta < 0 else place[axis] < sizes[axis] - 1)

    def along(g):
        return (place["depth"], g)

    def target(d):
        axis, delta = DIRS[d]
        there = dict(place)
        there[axis] = place[axis] + delta
        return (there["depth"], there["gx"])

    relayed = side > 1
    if relayed:
        column = lax.rem(me, side)
        cross = {2: has[2] & (column == 0), 3: has[3] & (column == side - 1)}
        via = {2: me - side, 3: me + side}
        serves = {
            2: (column == 0) & (me + side < lanes),
            3: (column == side - 1) & (me - side >= 0),
        }
        serve_from = {2: me + side, 3: me - side}
        serve_to = {2: me + side - 1, 3: me - side + 1}

    meets = [(has[d], target(d)) for d in range(4)]
    if relayed:
        for d in (2, 3):
            step_back = -side + 1 if d == 2 else side - 1
            back = me - step_back - (1 if d == 2 else -1)
            meets.append((cross[d], along(via[d])))
            meets.append((serves[d], along(serve_from[d])))
            if side > 2:
                meets.append((serves[d], along(serve_to[d])))
                meets.append((cross[d], along(me + (side - 1 if d == 2 else 1 - side))))

    barrier = pltpu.get_barrier_semaphore()
    for there, device in meets:
        @pl.when(there)
        def _():
            pl.semaphore_signal(barrier, inc=1, device_id=device, device_id_type=MESH)

    half = max(T, depth // 2 // T * T) if relayed else depth

    xs, zs = pl.ds(W, rows), pl.ds(T, depth)
    za, zb = pl.ds(T, half), pl.ds(T + half, depth - half)

    def load(source, buf, s, k):
        return pltpu.make_async_copy(
            source.at[s], grid.at[buf, s, xs, zs, :], load_sem.at[k, s]
        )

    def passed(r, s):
        if relayed:
            for d in wide:
                pl.when(serves[d] & bends(r, s))(lambda: forward(r, lax.rem(r, 2), s, d + 2).wait_send())

    for s in range(shots):
        load(now_hbm, 0, s, 0).start()
    scalars = [
        pltpu.make_async_copy(a, b, scalar_sem.at[i])
        for i, (a, b) in enumerate((
            (courant_hbm, courant), (cells_hbm, cells), (wavelet_hbm, wavelet),
            (start_hbm, start),
        ))
    ]
    for copy in scalars:
        copy.start()
    load_class = pltpu.make_async_copy(class_hbm, klass, class_sem)

    pieces = [
        (0, xs, pl.ds(T, ZL), xs, pl.ds(T + depth, ZL)),
        (1, xs, pl.ds(T + depth - ZL, ZL), xs, pl.ds(T - ZL, ZL)),
        (2, pl.ds(W, W), za, pl.ds(W + rows, W), za),
        (3, pl.ds(rows, W), za, pl.ds(0, W), za),
    ]
    if relayed:
        pieces += [
            (2, pl.ds(W, W), zb, pl.ds(W + rows, W), zb),
            (3, pl.ds(rows, W), zb, pl.ds(0, W), zb),
            (2, pl.ds(W, W), zs, pl.ds(W + rows, W), zs),
            (3, pl.ds(rows, W), zs, pl.ds(0, W), zs),
        ]

    def halo(buf, s, k):
        d, sx, sz, dx, dz = pieces[k]
        return pltpu.make_async_remote_copy(
            src_ref=grid.at[buf, s, sx, sz, :],
            dst_ref=grid.at[buf, s, dx, dz, :],
            send_sem=send_sem.at[buf, s, k],
            recv_sem=recv_sem.at[buf, s, k],
            device_id=target(d),
            device_id_type=MESH,
        )

    def detour(r, buf, s, k):
        d, sx, sz, _, _ = pieces[k]
        return pltpu.make_async_remote_copy(
            src_ref=grid.at[buf, s, sx, sz, :],
            dst_ref=relay.at[r, s],
            send_sem=send_sem.at[buf, s, k],
            recv_sem=relay_sem.at[r, s],
            device_id=along(via[d]),
            device_id_type=MESH,
        )

    def forward(r, buf, s, k):
        d, _, _, dx, dz = pieces[k]
        return pltpu.make_async_remote_copy(
            src_ref=relay.at[r, s],
            dst_ref=grid.at[buf, s, dx, dz, :],
            send_sem=forward_sem.at[r, s],
            recv_sem=recv_sem.at[buf, s, k],
            device_id=along(serve_to[d]),
            device_id_type=MESH,
        )

    for d in range(4):
        _, _, _, dx, dz = pieces[d ^ 1]
        if d >= 2:
            dz = zs

        @pl.when(jnp.logical_not(has[d]))
        def _():
            for buf in range(2):
                def clear(s, c):
                    shape = (dx.size, dz.size, width)
                    grid[buf, s, dx, dz, :] = jnp.zeros(shape, jnp.float32)
                    return c
                lax.fori_loop(0, shots, clear, 0)

    peers = sum(there.astype(jnp.int32) for there, _ in meets)
    pl.semaphore_wait(barrier, peers)

    def bends(r, s):
        last = (r == iters - 1) & (s == shots - 1)
        return jnp.logical_not(last)

    def each(ways, straight, around, bend=True):
        for d in ways:
            if d < 2 or not relayed:
                pl.when(has[d])(lambda: straight(d))
                continue

            @pl.when(cross[d] & bend)
            def _():
                around(d + 2)
                straight(d)

            pl.when(has[d] & jnp.logical_not(cross[d] & bend))(lambda: straight(d + 4))

    wide = (2, 3)

    def send(r, buf, s, ways):
        each(ways, lambda k: halo(buf, s, k).start(), lambda k: detour(r, buf, s, k).start(),
             bends(r, s))

    def send_around(r, buf, s):
        if relayed:
            for d in wide:
                pl.when(cross[d])(lambda: detour(r, buf, s, d + 2).start())

    def send_straight(r, buf, s):
        each(wide, lambda k: halo(buf, s, k).start(), lambda k: None)

    def wait_sent(r, buf, s, ways):
        each(ways, lambda k: halo(buf, s, k).wait_send(),
             lambda k: detour(0, buf, s, k).wait_send(), bends(r, s))

    def wait_halo(r, buf, s, ways):
        for d in ways:
            if d < 2 or not relayed:
                pl.when(has[d ^ 1])(lambda: halo(buf, s, d).wait_recv())
                continue

            bend = bends(r, s)

            @pl.when(cross[d ^ 1] & bend)
            def _():
                halo(buf, s, d).wait_recv()
                halo(buf, s, d + 2).wait_recv()

            plain = has[d ^ 1] & jnp.logical_not(cross[d ^ 1] & bend)
            pl.when(plain)(lambda: halo(buf, s, d + 4).wait_recv())

    def pass_on(r, s):
        if not relayed:
            return
        for k in (4, 5):
            @pl.when(serves[pieces[k][0]] & bends(r, s))
            def _():
                buf = r % 2 if isinstance(r, int) else lax.rem(r, 2)
                detour(r, buf, s, k).wait_recv()
                forward(r, buf, s, k).start()

    lag = min(LAG, shots)
    early = min(lag, shots)
    for s in range(early):
        load(now_hbm, 0, s, 0).wait()
        send(0, 0, s, wide)
    for s in range(early, shots):
        load(now_hbm, 0, s, 0).wait()
        send_around(0, 0, s)
    for s in range(shots):
        send(0, 0, s, (0, 1))
    load_class.start()
    for s in range(shots):
        load(before_hbm, 1, s, 1).start()

    for copy in scalars:
        copy.wait()
    z_index = place["depth"] * depth + lax.broadcasted_iota(jnp.int32, (depth, width), 0)
    total = depth * sizes["depth"]
    begin = jnp.full((depth, width), start[0, 0], jnp.int32)
    ratio = (z_index - begin + 1).astype(jnp.float32) / (total - begin).astype(jnp.float32)
    damping = jnp.where(z_index >= begin, DAMPING * ratio * ratio, jnp.float32(0.0))
    inverse = 1.0 / (1.0 + damping)
    scale[0] = inverse
    scale[1] = 2.0 * inverse

    load_class.wait()

    def lookup(x, c):
        held = klass[x]
        value = jnp.zeros((depth, width), jnp.float32)
        for k in range(classes):
            value = jnp.where(held == k, courant[k], value)
        speed[x] = value * scale[0]
        return c

    lax.fori_loop(0, rows, lookup, 0)
    for s in range(shots):
        load(before_hbm, 1, s, 1).wait()

    for s in range(early, shots):
        pass_on(0, s - early)
        send_straight(0, 0, s)

    lane = lax.broadcasted_iota(jnp.int32, (T, width), 1)
    low = [jnp.where(lane >= k, jnp.float32(COEFFS[k]), 0.0) for k in range(1, W + 1)]
    high = [jnp.where(lane < width - k, jnp.float32(COEFFS[k]), 0.0) for k in range(1, W + 1)]
    x_anchor = place["gx"] * rows

    group = math.gcd(rows, GROUP)

    def compute(t, s, buf, other):
        lane_z = lax.broadcasted_iota(jnp.int32, (depth, width), 1)
        hit = (z_index == cells[s, 1]) & (lane_z == cells[s, 2])
        pulse = jnp.where(hit, wavelet[s, t] * scale[0], 0.0)
        cell_x = cells[s, 0] - x_anchor

        def block_of(x, j, above, below):
            z = T + j * T

            def at(dx, dz):
                return grid[buf, s, x + W + dx, pl.ds(z + dz, T), :]

            p = at(0, 0)
            lap = (3.0 * COEFFS[0]) * p
            for k in range(1, W + 1):
                pair = at(0, k) + at(0, -k)
                if k <= above:
                    pair = pair + at(-k, 0)
                if k <= below:
                    pair = pair + at(k, 0)
                lap = lap + COEFFS[k] * pair
                lap = lap + (
                    low[k - 1] * pltpu.roll(p, k, 1)
                    + high[k - 1] * pltpu.roll(p, width - k, 1)
                )
            q = grid[other, s, x + W, pl.ds(z, T), :]
            block = pl.ds(j * T, T)
            nxt = scale[1, block, :] * (p - q) + q + speed[x, block, :] * lap
            amp = jnp.where(x == cell_x, jnp.float32(1.0), jnp.float32(0.0))
            return nxt + amp * pulse[j * T : (j + 1) * T]

        def run(begin, top, bottom):
            spots = [(i, j) for i in range(group) for j in range(depth // T)]
            values = [
                block_of(begin + i, j, i if top else W, group - 1 - i if bottom else W)
                for i, j in spots
            ]
            for (i, j), value in zip(spots, values):
                grid[other, s, begin + i + W, pl.ds(T + j * T, T), :] = value

        count = rows // group
        run(0, True, count == 1)
        if count > 1:
            run(rows - group, False, True)

        def row(g, c):
            run(g * group, False, False)
            return c

        lax.fori_loop(1, count - 1, row, 0)

    def complete(s, buf, other):
        for j in range(depth // T):
            z = pl.ds(T + j * T, T)
            block = pl.ds(j * T, T)
            ahead = [grid[buf, s, W - 1 - k, z, :] for k in range(W)]
            after = [grid[buf, s, W + rows + k, z, :] for k in range(W)]
            for i in range(W):
                for x, beyond in ((i, ahead), (rows - 1 - i, after)):
                    lap = COEFFS[i + 1] * beyond[0]
                    for k in range(1, W - i):
                        lap = lap + COEFFS[i + 1 + k] * beyond[k]
                    partial = grid[other, s, x + W, z, :]
                    grid[other, s, x + W, z, :] = partial + speed[x, block, :] * lap

    def step(t, c):
        buf = lax.rem(t, 2)
        other = 1 - buf

        def shot(s, c):
            wait_halo(t, buf, s, (0, 1))
            compute(t, s, buf, other)
            wait_sent(t, buf, s, (0, 1) + wide)
            passed(t, s)

            unit = t * shots + s + shots - lag
            r, u = unit // shots, lax.rem(unit, shots)
            pl.when(r < iters)(lambda: pass_on(r, u))

            wait_halo(t, buf, s, wide)
            complete(s, buf, other)

            @pl.when(t < iters - 1)
            def _():
                send(t + 1, other, s, wide + (0, 1))

            return c

        return lax.fori_loop(0, shots, shot, c)

    lax.fori_loop(0, iters, step, 0)


def put_out(iters, shots, rows, depth, grid, final_hbm, prior_hbm, out_sem):
    xs, zs = pl.ds(W, rows), pl.ds(T, depth)
    copies = [
        pltpu.make_async_copy(grid.at[buf, s, xs, zs, :], out.at[s], out_sem.at[k, s])
        for s in range(shots)
        for k, (buf, out) in enumerate(((iters % 2, final_hbm), (1 - iters % 2, prior_hbm)))
    ]
    for copy in copies:
        copy.start()
    for copy in copies:
        copy.wait()


def solution(mesh):
    sizes = {axis: mesh.shape[axis] for axis in ("depth", "gx")}
    side = math.isqrt(sizes["gx"])
    if side * side != sizes["gx"]:
        side = 0

    def local(now, before, class_map, courant, cells, wavelet, start):
        shots, rows, depth, width = now.shape
        iters = wavelet.shape[0]
        split = side if depth >= 2 * T else 0
        body = functools.partial(
            kernel, sizes, split, iters, shots, rows, depth, width, courant.shape[0]
        )
        whole = pl.BlockSpec(memory_space=pl.ANY)
        far = pl.BlockSpec(memory_space=pltpu.HBM)
        out = jax.ShapeDtypeStruct(now.shape, jnp.float32)
        half = max(T, depth // 2 // T * T)
        operands = [
            pltpu.with_memory_space_constraint(a, pltpu.HBM)
            for a in (now, before, class_map, courant, cells, wavelet.T)
        ]
        grid = pl.pallas_call(
            body,
            out_shape=pltpu.VMEM(
                (2, shots, rows + 2 * W, depth + 2 * T, width), jnp.float32
            ),
            in_specs=[far] * len(operands) + [whole],
            out_specs=pl.BlockSpec(memory_space=pltpu.VMEM),
            scratch_shapes=[
                pltpu.SMEM(courant.shape, courant.dtype),
                pltpu.SMEM(cells.shape, cells.dtype),
                pltpu.SMEM(wavelet.shape[::-1], wavelet.dtype),
                pltpu.SMEM((1, 1), start.dtype),
                pltpu.SemaphoreType.DMA((4,)),
                pltpu.VMEM((iters, shots, W, depth - half, width), jnp.float32),
                pltpu.VMEM((rows, depth, width), jnp.float32),
                pltpu.VMEM((2, depth, width), jnp.float32),
                pltpu.VMEM((rows, depth, width), jnp.int32),
                pltpu.SemaphoreType.DMA((2, shots)),
                pltpu.SemaphoreType.DMA,
                pltpu.SemaphoreType.DMA((2, shots, 8)),
                pltpu.SemaphoreType.DMA((2, shots, 8)),
                pltpu.SemaphoreType.DMA((iters, shots)),
                pltpu.SemaphoreType.DMA((iters, shots)),
            ],
            compiler_params=pltpu.CompilerParams(
                collective_id=0, has_side_effects=True, vmem_limit_bytes=16 * 1024 * 1024
            ),
            name="wave",
        )(*operands, start.reshape(1, 1))
        grid = pltpu.with_memory_space_constraint(grid, pltpu.VMEM)
        return pl.pallas_call(
            functools.partial(put_out, iters, shots, rows, depth),
            out_shape=(out, out),
            in_specs=[whole],
            out_specs=(whole, whole),
            scratch_shapes=[pltpu.SemaphoreType.DMA((2, shots))],
            compiler_params=pltpu.CompilerParams(vmem_limit_bytes=1024 * 1024),
            name="put_out",
        )(grid)

    placed = P(None, "gx", "depth", None)
    return jax.shard_map(
        local,
        mesh=mesh,
        in_specs=(placed, placed, P("gx", "depth", None), P(), P(), P(), P()),
        out_specs=(placed, placed),
        check_vma=False,
    )
```
